256 devices in a mesh: rep: 4 (over z_hi), tok: 4 (over z_lo, core), voc: 16 (over x, y).
Axes of the slice: x: 4, y: 4, z: 8 (z_hi: 4, z_lo: 2; z = z_hi * 2 + z_lo), core: 2. Of those that a mesh axis runs over, the one named last changes fastest.
Arguments:
- hidden: bfloat16 [4, 512, 4096], P('rep', ('tok', 'voc')), may hold values from -500 to 500
- targets: int32 [4, 512], P('rep', ('tok', 'voc')), may hold values from 0 to 65535
- unembed: bfloat16 [4, 65536, 4096], P('rep', ('tok', 'voc')), may hold values from -1 to 1
- outer_weight: float32 [8192, 4096], P(('tok', 'voc'), 'rep'), may hold values from -0.9 to 0.9
- momentum: float32 [8192, 4096], P(('tok', 'voc'), 'rep'), may hold values from -0.18 to 0.18
Outputs:
- token_loss: float32 [4, 512], P('rep', ('tok', 'voc'))
- hidden_grad: float32 [4, 512, 4096], P('rep', ('tok', 'voc'))
- new_outer: float32 [8192, 4096], P(('tok', 'voc'), 'rep')
- new_momentum: float32 [8192, 4096], P(('tok', 'voc'), 'rep')
- next_inner: bfloat16 [8192, 4096], P(('tok', 'voc'))
The draws below stay inside these ranges and needn't reach their ends.
All inputs are finite; a program needn't handle non-finite values.
Results may differ from the reference program's by a relative error of at most 0.0085.
Values may be sent and summed in bfloat16 or wider, within the bound.
No kernel may reach another device: no remote copies, remote signals or barrier semaphores. Data moves between devices by JAX's collectives and lax.ppermute only.
A program may use at most 64 MiB of HBM per device.

```python
import math
import jax
import jax.numpy as jnp
import numpy as np
from jax import lax

D = 4096
VOC_DEV = 1024
SLAB_DEV = 128
REPLICAS = 4
TOKENS = 512
VOCAB = 65536
SLAB = 8192


weight_scale = 0.15


state_scale = 20.0


def base_rows(key, row_ids):
    base_key = jax.random.fold_in(key, 101)

    def one_row(row):
        noise = jax.random.normal(jax.random.fold_in(base_key, row), (D,), jnp.float32)
        return weight_scale * jnp.clip(noise, -6.0, 6.0)
    return jax.vmap(one_row)(row_ids)


def inner_rows(key, replica, row_ids):
    drift_key = jax.random.fold_in(key, 202)

    def one_row(row):
        noise = jax.random.normal(jax.random.fold_in(drift_key, replica * VOCAB + row), (D,), jnp.float32)
        return 0.1 * weight_scale * jnp.clip(noise, -6.0, 6.0)
    return base_rows(key, row_ids) + jax.vmap(one_row)(row_ids)


def draw_unembed(key, part):
    row_ids = jnp.arange(VOCAB, dtype=jnp.int32)

    def one_replica(replica):
        return inner_rows(key, replica, row_ids).astype(jnp.bfloat16)
    return lax.map(one_replica, jnp.arange(REPLICAS, dtype=jnp.int32))


def draw_outer_weight(key, part):
    slab_index = jnp.arange(SLAB, dtype=jnp.int32)
    row_ids = slab_index // SLAB_DEV * VOC_DEV + slab_index % SLAB_DEV
    return base_rows(key, row_ids)


def draw_hidden(key, part):
    noise = jnp.clip(jax.random.normal(jax.random.fold_in(key, 303), (REPLICAS, TOKENS, D), jnp.float32), -6.0, 6.0)
    return (state_scale * noise).astype(jnp.bfloat16)


def place_ends(drawn, rng, least, high):
    shape = drawn.shape
    spot = [jax.random.randint(jax.random.fold_in(rng, axis), (), 0, shape[axis]) for axis in range(len(shape))]
    drawn = drawn.at[tuple(spot)].set(least)
    longest = shape.index(max(shape))
    spot[longest] = (spot[longest] + 1) % shape[longest]
    return drawn.at[tuple(spot)].set(high)


def block_levels(stream_key, dims, split, low, high):
    loudness = 1.0
    for position, blocks in split:
        steps = jax.random.uniform(jax.random.fold_in(jax.random.fold_in(stream_key, 6), position), (blocks,), jnp.float32, low / len(split), high / len(split))
        loudness = loudness * jnp.repeat(jnp.exp(steps), dims[position] // blocks).reshape((-1,) + (1,) * (len(dims) - 1 - position))
    return loudness


def rank_table(number_of, lean):
    weights = [(1 << 20) // math.isqrt(grade ** lean) + 1 for grade in range(1, number_of + 1)]
    spread = 1 + sum(weights) // (1 << 30)
    return np.cumsum(np.array([max(1, weight // spread) for weight in weights]))


def skewed_ids(own_key, shape, count, lean):
    table = rank_table(count, lean)
    pick = jax.random.randint(jax.random.fold_in(own_key, 1), shape, 0, int(table[count - 1]))
    standing = jnp.searchsorted(jnp.asarray(table, jnp.int32), pick, side="right")
    return jax.random.permutation(jax.random.fold_in(own_key, 2), count)[standing].astype(jnp.int32)


def centred(rng, shape, deviation, bound, shards=(), held_as=jnp.bfloat16):
    gain = block_levels(rng, shape, shards, -0.22, 0.18) if shards else 1.0
    array = jax.random.normal(rng, shape, jnp.float32) * deviation * gain
    return jnp.minimum(jnp.maximum(array, -bound), bound).astype(held_as)


def setup_inputs(seed: int = 0) -> dict:
    splits = jax.random.split(jax.random.key(seed), 6)
    hidden = draw_hidden(jax.random.fold_in(splits[5], 71), 0)
    targets = place_ends(skewed_ids(splits[1], (REPLICAS, TOKENS), VOCAB, 2), jax.random.fold_in(splits[1], 3), 0, VOCAB - 1).astype(jnp.int32)
    unembed = draw_unembed(jax.random.fold_in(splits[5], 71), 0)
    outer_weight = draw_outer_weight(jax.random.fold_in(splits[5], 71), 0)
    momentum = centred(splits[4], (SLAB, D), 0.03, 0.18, ((0, 64), (1, 4)), jnp.float32)
    return {"hidden": hidden, "targets": targets, "unembed": unembed, "outer_weight": outer_weight, "momentum": momentum}


inner_rate = 0.5
outer_rate = 0.7
momentum_coef = 0.9


def replica_step(inputs):
    states, labels, weights = inputs
    model_width = states.shape[1]
    logit_scale = model_width ** -0.5
    vocab_size = weights.shape[0]
    logits = jnp.dot(states, weights.T, preferred_element_type=jnp.float32) * logit_scale
    row_top = jnp.max(logits, axis=1)
    log_total = row_top + jnp.log(jnp.sum(jnp.exp(logits - row_top[:, None]), axis=1))
    onehot = labels[:, None] == jnp.arange(vocab_size, dtype=jnp.int32)[None, :]
    target_logit = jnp.sum(jnp.where(onehot, logits, 0.0), axis=1)
    token_loss = log_total - target_logit
    errors = (jnp.exp(logits - log_total[:, None]) - onehot.astype(jnp.float32)).astype(jnp.bfloat16)
    hidden_grad = jnp.dot(errors, weights, preferred_element_type=jnp.float32) * logit_scale
    slab_index = jnp.arange(SLAB, dtype=jnp.int32)
    slab_rows = (slab_index // SLAB_DEV) * VOC_DEV + slab_index % SLAB_DEV
    slab_errors = jnp.take(errors, slab_rows, axis=1)
    slab_grad = jnp.dot(slab_errors.T, states, preferred_element_type=jnp.float32) * logit_scale
    final_slab = jnp.take(weights, slab_rows, axis=0).astype(jnp.float32) - inner_rate * slab_grad
    return token_loss, hidden_grad, final_slab


def reference(hidden, targets, unembed, outer_weight, momentum):
    token_loss, hidden_grad, final_slab = lax.map(replica_step, (hidden, targets, unembed))
    mean_final = jnp.mean(final_slab, axis=0)
    pseudo_grad = outer_weight - mean_final
    new_momentum = momentum_coef * momentum + pseudo_grad
    new_outer = outer_weight - outer_rate * (pseudo_grad + momentum_coef * new_momentum)
    next_inner = new_outer.astype(jnp.bfloat16)
    return token_loss, hidden_grad, new_outer, new_momentum, next_inner
```

```python
import jax
import jax.numpy as jnp
from jax import lax
from jax.sharding import Mesh
from jax.sharding import PartitionSpec as P

TOK = ("tok_0", "tok_1")
VOC = ("voc_0", "voc_1")
TOK_VOC = ("tok_0", "tok_1", "voc_0", "voc_1")
Z, CORE, X, Y = TOK_VOC


inner_rate = 0.5
outer_rate = 0.7
momentum_coef = 0.9


def take(value, axis, k):
    n = lax.axis_size(axis)
    return lax.ppermute(value, axis, [((i + k) % n, i) for i in range(n)])


def ring_gather(value, axis):
    half = value.shape[0] // 2
    up, down = take(value, axis, 1), take(value, axis, -1)
    far = (take(up[:half], axis, 1), take(down[half:], axis, -1))
    return value, up, jnp.concatenate(far), down


def direct_gather(value, axis):
    return value, take(value, axis, 1), take(value, axis, 2), take(value, axis, -1)


def spread(piece):
    other = take(piece, Z, 1)
    along_x = jnp.concatenate(direct_gather(piece, X))
    along_y = jnp.concatenate(direct_gather(other, Y))
    near = ring_gather(along_x, Y)
    far = ring_gather(along_y, X)
    near, far = jnp.concatenate(near), jnp.concatenate(far)
    return (near, far, take(near, CORE, 1), take(far, CORE, 1))


def to_f32(value):
    return value.astype(jnp.float32)


def ring_reduce(pieces, axis):
    here, up, across, down = pieces
    half = across.shape[0] // 2
    from_up = take(across[half:], axis, 1)
    from_down = take(across[:half], axis, -1)
    up = jnp.concatenate((to_f32(up[:half]) + to_f32(from_down), to_f32(up[half:])))
    down = jnp.concatenate((to_f32(down[:half]), to_f32(down[half:]) + to_f32(from_up)))
    got = (take(up.astype(jnp.bfloat16), axis, -1), take(down.astype(jnp.bfloat16), axis, 1))
    return to_f32(here) + to_f32(got[0]) + to_f32(got[1])


def direct_reduce(pieces, axis):
    total = to_f32(pieces[0])
    for k in (1, 2, 3):
        total = total + to_f32(take(pieces[k], axis, -k))
    return total


def combined(stats, others):
    tops = [part[0] for part in (stats, *others)]
    top = tops[0]
    for one in tops[1:]:
        top = jnp.maximum(top, one)
    total = sum(part[1] * jnp.exp(part[0] - top) for part in (stats, *others))
    target = sum(part[2] for part in (stats, *others))
    return jnp.stack((top, total, target))


def gathered_stats(stats):
    group = lambda k: lax.ppermute(stats, TOK, [(i ^ k, i) for i in range(4)])
    stats = combined(
        stats, (group(1)[:, ::-1], group(2)[:, :, ::-1], group(3)[:, ::-1, ::-1])
    )
    for axis, dim in ((X, 4), (Y, 3)):
        stats = combined(stats, [jnp.roll(take(stats, axis, k), k, dim) for k in (1, 2, 3)])
    return stats


def nesterov(outer_part, momentum_part, mean_final):
    pseudo_grad = outer_part - mean_final
    moved_momentum = momentum_coef * momentum_part + pseudo_grad
    moved_outer = outer_part - outer_rate * (pseudo_grad + momentum_coef * moved_momentum)
    return (moved_outer, moved_momentum)


def per_device(hidden, targets, unembed, outer_weight, momentum):
    weights = unembed[0]
    vocab_rows, width = weights.shape
    own = hidden.shape[1]
    slab_rows, part = outer_weight.shape
    reps = lax.axis_size("rep")
    rep = lax.axis_index("rep")
    scale = width ** (-0.5)
    group_index = lax.axis_index(TOK) * lax.axis_size(VOC) + lax.axis_index(VOC)

    def features(value, k):
        return lax.dynamic_slice_in_dim(value, ((rep + k) % reps) * part, part, 1)

    ids = targets[0]
    codes = jnp.stack((ids >> 8, ids & 255), 1).astype(jnp.bfloat16)
    piece = jnp.concatenate((hidden[0], jnp.pad(codes, ((0, 0), (0, 126)))), 1)
    got = spread(piece)
    every = jnp.concatenate([p[:, :width] for p in got])
    codes = jnp.concatenate([p[:, width : width + 2] for p in got]).astype(jnp.int32)
    every_target = codes[:, 0] * 256 + codes[:, 1]
    tokens = every.shape[0]

    foreign = [
        lax.ppermute(features(hidden[0], -k), "rep", [((i + k) % reps, i) for i in range(reps)])
        for k in (1, 2, 3)
    ]
    foreign = spread(jnp.concatenate(foreign, 1))
    slab = weights[:slab_rows]
    mean_weight = to_f32(features(slab, 0))
    for k in (1, 2, 3):
        mean_weight = mean_weight + to_f32(take(features(slab, -k), "rep", k))
    mean_weight = mean_weight / reps

    logits = (
        jnp.einsum("td,vd->tv", every, weights, preferred_element_type=jnp.float32) * scale
    )
    columns = group_index * vocab_rows + lax.broadcasted_iota(jnp.int32, (1, vocab_rows), 1)
    onehot = every_target[:, None] == columns
    stats = jnp.stack(
        (
            top := jnp.max(logits, axis=1),
            jnp.sum(jnp.exp(logits - top[:, None]), axis=1),
            jnp.sum(jnp.where(onehot, logits, 0.0), axis=1),
        )
    )
    stats = stats.reshape(3, 2, 2, 4, 4, own)
    stats = jnp.stack((stats[:, :, 0], jnp.swapaxes(stats[:, :, 1], 2, 3)), 2)
    top, total, target_logit = gathered_stats(stats)
    log_total = top + jnp.log(total)
    token_loss = (log_total - target_logit)[0, 0, 0, 0][None]
    log_total = jnp.stack((log_total[:, 0], jnp.swapaxes(log_total[:, 1], 1, 2)), 1).reshape(tokens, 1)

    errors = (jnp.exp(logits - log_total) - onehot.astype(jnp.float32)).astype(jnp.bfloat16)

    slab_errors = ring_gather(errors[:, :slab_rows], "rep")
    states = [features(every, 0)] + [
        jnp.concatenate([p[:, k * part : (k + 1) * part] for p in foreign]) for k in range(3)
    ]
    slab_grad = sum(
        jnp.einsum("tv,td->vd", e, h, preferred_element_type=jnp.float32)
        for e, h in zip(slab_errors, states)
    )
    mean_final = mean_weight - (inner_rate * scale / reps) * slab_grad
    new_outer, new_momentum = nesterov(outer_weight, momentum, mean_final)
    pieces = ring_gather(new_outer.astype(jnp.bfloat16), "rep")
    next_inner = jnp.zeros((slab_rows, width), jnp.bfloat16)
    for k in range(4):
        next_inner = lax.dynamic_update_slice(
            next_inner, pieces[k], (0, ((rep + k) % reps) * part)
        )

    grad = (jnp.dot(errors, weights, preferred_element_type=jnp.float32) * scale).astype(
        jnp.bfloat16
    )
    half = tokens // 2
    quarter = half // 2
    near = to_f32(grad[:quarter]) + to_f32(take(grad[half : half + quarter], CORE, 1))
    far = to_f32(grad[quarter:half]) + to_f32(take(grad[half + quarter :], CORE, 1))
    near = near.astype(jnp.bfloat16).reshape(4, 4 * own, width)
    far = far.astype(jnp.bfloat16).reshape(4, 4 * own, width)
    near = ring_reduce(near, Y).astype(jnp.bfloat16).reshape(4, own, width)
    far = ring_reduce(far, X).astype(jnp.bfloat16).reshape(4, own, width)
    near, far = direct_reduce(near, X), direct_reduce(far, Y)
    token_grad = near + to_f32(take(far.astype(jnp.bfloat16), Z, 1))
    return (token_loss, token_grad[None], new_outer, new_momentum, next_inner)


def solution(mesh):
    finer = Mesh(
        mesh.devices.reshape(mesh.shape["rep"], 2, 2, 4, 4),
        ("rep", "tok_0", "tok_1", "voc_0", "voc_1"),
    )
    in_specs = (
        P("rep", TOK_VOC, None),
        P("rep", TOK_VOC),
        P("rep", TOK_VOC, None),
        P(TOK_VOC, "rep"),
        P(TOK_VOC, "rep"),
    )
    out_specs = (
        P("rep", TOK_VOC),
        P("rep", TOK_VOC, None),
        P(TOK_VOC, "rep"),
        P(TOK_VOC, "rep"),
        P(TOK_VOC, None),
    )
    return jax.shard_map(
        per_device, mesh=finer, in_specs=in_specs, out_specs=out_specs, check_vma=False
    )
```

```python
import functools

import jax
import jax.numpy as jnp
from jax import lax
from jax.experimental import pallas as pl
from jax.experimental.pallas import tpu as pltpu
from jax.sharding import Mesh
from jax.sharding import PartitionSpec as P

TOK = ("tok_0", "tok_1")
VOC = ("voc_0", "voc_1")
TOK_VOC = ("tok_0", "tok_1", "voc_0", "voc_1")
Z, CORE, X, Y = TOK_VOC
F32, BF16 = jnp.float32, jnp.bfloat16

PARTS = (
    (0, 0, 0, 4), (1, 0, 0, 4),
    (0, 1, 0, 4), (0, 3, 0, 4), (1, 1, 0, 4), (1, 3, 0, 4),
    (0, 2, 0, 2), (0, 2, 2, 2), (1, 2, 0, 2), (1, 2, 2, 2),
)


inner_rate = 0.5
outer_rate = 0.7
momentum_coef = 0.9
SMEM = pl.BlockSpec(memory_space=pltpu.SMEM)
VMEM = pl.BlockSpec(memory_space=pltpu.VMEM)


def call(kernel, out, *operands, flops=0, scratch=(), limit=16, specs={}):
    moved = sum(leaf.size * leaf.dtype.itemsize for leaf in jax.tree.leaves((operands, out)))
    return pl.pallas_call(
        kernel,
        in_specs=[SMEM] + [specs.get(k, VMEM) for k in range(1, len(operands))],
        out_specs=jax.tree.map(lambda _: VMEM, out),
        out_shape=out,
        scratch_shapes=scratch,
        compiler_params=pltpu.CompilerParams(vmem_limit_bytes=limit << 20),
        cost_estimate=pl.CostEstimate(
            flops=flops or moved, bytes_accessed=moved, transcendentals=0
        ),
    )(*operands)


def shaped(dtype, *shape):
    return jax.ShapeDtypeStruct(shape, dtype)


def by_core(k, inner):
    pairs = []
    for core in range(2):
        for x in range(4):
            for y in range(4):
                along_x = (core == 1) != inner
                fx, fy = ((x + k) % 4, y) if along_x else (x, (y + k) % 4)
                pairs.append(((core * 4 + fx) * 4 + fy, (core * 4 + x) * 4 + y))
    return pairs


def take_outer(value, k):
    return lax.ppermute(value, (CORE, X, Y), by_core(k, False))


def take_inner(value, k):
    return lax.ppermute(value, (CORE, X, Y), by_core(k, True))


def take(value, axis, k):
    n = lax.axis_size(axis)
    return lax.ppermute(value, axis, [((i + k) % n, i) for i in range(n)])


def along(axis):
    return lambda value, k: take(value, axis, k)


def ring_gather(value, take):
    half = value.shape[0] // 2
    up, down = take(value, 1), take(value, -1)
    far = (take(up[:half], 1), take(down[half:], -1))
    return value, up, *far, down


def to_f32(value):
    return value.astype(F32)


def ring_reduce(pieces, take):
    here, up, first, second, down = pieces
    half = first.shape[0]
    from_up = take(second, 1)
    from_down = take(first, -1)
    up = jnp.concatenate((to_f32(up[:half]) + to_f32(from_down), to_f32(up[half:])))
    down = jnp.concatenate((to_f32(down[:half]), to_f32(down[half:]) + to_f32(from_up)))
    up = take(up.astype(BF16), -1)
    down = take(down.astype(BF16), 1)
    return here, up, down


def part_tokens(here, own, other, a, first, count):
    row = lax.broadcasted_iota(jnp.int32, (count * 2 * own, 1), 0)
    t, plane, b = row % own, row // own % 2, row // (2 * own) + first
    z, c = (here[0] + plane) % 2, (here[1] + other) % 2
    x = (here[2] + jnp.where(c == 0, b, a)) % 4
    y = (here[3] + jnp.where(c == 0, a, b)) % 4
    return (((z * 2 + c) * 4 + x) * 4 + y) * own + t


def token_table(here, tokens, own):
    lane = lax.broadcasted_iota(jnp.int32, (1, tokens), 1)
    rows = [
        part_tokens(here, own, other, a, first, count) == lane for other, a, first, count in PARTS
    ]
    return jnp.concatenate([one.astype(F32) for one in rows]).astype(BF16)


def in_three(value):
    high = value.astype(BF16)
    rest = value - high.astype(F32)
    middle = rest.astype(BF16)
    return high, middle, (rest - middle.astype(F32)).astype(BF16)


def reordered(value, table, dims):
    dot = lambda one: lax.dot_general(one, table, (dims, ((), ())), preferred_element_type=F32)
    return sum(dot(one) for one in in_three(value))


def logits_kernel(own, count, before, here, *refs):
    parts, refs = refs[:count], refs[count:]
    first = not before
    w_in, tables, (logits, ids, states, table, *more) = refs[0], refs[1 : 1 + before], refs[1 + before :]
    w = more[0] if first else w_in
    vocab_rows, width = w.shape
    block = 256

    def copy(k):
        at = pl.ds(k * block, block)
        return pltpu.make_async_copy(w_in.at[at, :], w.at[at, :], more[1].at[k])

    if first:
        for k in range(vocab_rows // block):
            copy(k).start()
    start = 0
    for part in parts:
        at = pl.ds(start, part.shape[0])
        states[at, :] = part[:, :width]
        codes = part[:, width:].astype(F32).astype(jnp.int32)
        ids[at, :] = codes[:, :1] * 256 + codes[:, 1:2]
        start += part.shape[0]
    if first:
        for k in range(vocab_rows // block):
            copy(k).wait()
    rows = states.shape[0]
    lane = lax.broadcasted_iota(jnp.int32, (1, 128), 1)

    def step(j, carry):
        top, total, target = carry
        column = pl.multiple_of(j * block, block)
        out = lax.dot_general(
            states[...], w[pl.ds(column, block), :], (((1,), (1,)), ((), ())),
            preferred_element_type=F32,
        ) * (width ** (-0.5))
        logits[:, pl.ds(column, block)] = out
        hits = ids[...] - (here[4] + column)
        lanes = [out[:, k : k + 128] for k in range(0, block, 128)]
        peak = top
        for one in lanes:
            peak = jnp.maximum(peak, one)
        total = total * jnp.exp(top - peak)
        for k, one in enumerate(lanes):
            total = total + jnp.exp(one - peak)
            target = target + jnp.where(hits - k * 128 == lane, one, 0.0)
        return peak, total, target

    zero = jnp.zeros((rows, 128), F32)
    peak, total, target = lax.fori_loop(
        0, vocab_rows // block, step, (jnp.full((rows, 128), -jnp.inf, F32), zero, zero)
    )
    best = jnp.max(peak, axis=1, keepdims=True)
    mass = jnp.sum(total * jnp.exp(peak - best), axis=1, keepdims=True)
    hit = jnp.sum(target, axis=1, keepdims=True)
    mine = jnp.where(lane == 0, best, jnp.where(lane == 1, mass, jnp.where(lane == 2, hit, 0.0)))
    if before < 2:
        table[...] = mine
    else:
        every = jnp.concatenate([one[...] for one in tables] + [mine])
        table[...] = reordered(every, token_table(here, every.shape[0], own), ((0,), (0,)))[:8]


def merged(parts):
    top = parts[0][0:1]
    for one in parts[1:]:
        top = jnp.maximum(top, one[0:1])
    total = sum(one[1:2] * jnp.exp(one[0:1] - top) for one in parts)
    return top, total, sum(one[2:3] for one in parts)


def merge_kernel(here, *refs):
    got, out = refs[:-1], refs[-1]
    got = [got[0][k] for k in range(4)] if len(got) == 1 else [one[...] for one in got]
    top, total, target = merged(got)
    row = lax.broadcasted_iota(jnp.int32, out.shape, 0)
    out[...] = jnp.where(row == 0, top, jnp.where(row == 1, total, jnp.where(row == 2, target, 0.0)))


def slab_kernel(own, part, here, *refs):
    got, logits, ids, states, outs = refs[:4], refs[4:7], refs[7:10], refs[10:13], refs[13:]
    loss, log_total, mine, up, first, second, down, errors = outs
    tokens = errors.shape[0]
    width = 4 * part
    top, total, target = merged([one[...] for one in got])
    every = top + jnp.log(total)
    row = lax.broadcasted_iota(jnp.int32, got[0].shape, 0)
    both = jnp.where(row == 0, every, jnp.where(row == 1, every - target, 0.0))
    table = token_table(here, tokens, own)
    columns = sum(
        lax.dot_general(table, one, (((1,), (1,)), ((), ())), preferred_element_type=F32)
        for one in in_three(both)
    )
    log_total[...] = columns[:, 0:1]
    loss[...] = columns[:own, 1:2]
    strip = mine.shape[0]
    lane = lax.broadcasted_iota(jnp.int32, (1, strip), 1)
    start = 0
    for values, id_part in zip(logits, ids):
        end = start + values.shape[0]
        onehot = (id_part[...] - here[4] == lane).astype(F32)
        errors[start:end, :] = (
            jnp.exp(values[:, :strip] - columns[start:end, 0:1]) - onehot
        ).astype(BF16)
        start = end

    def grad(k):
        at = pl.multiple_of(lax.rem(here[5] + k, 4) * part, part)
        total, start = 0.0, 0
        for state in states:
            end = start + state.shape[0]
            total += lax.dot_general(
                errors[start:end, :], state[:, pl.ds(at, part)], (((0,), (0,)), ((), ())),
                preferred_element_type=F32,
            )
            start = end
        return total * (width ** (-0.5))

    half = first.shape[0]
    across = grad(2).astype(BF16)
    first[...], second[...] = across[:half], across[half:]
    up[...] = grad(1).astype(BF16)
    down[...] = grad(3).astype(BF16)
    mine[...] = grad(0)


def hidden_kernel(here, *refs):
    logits, ids, (log_total, w, keep, send, errors) = refs[:3], refs[3:6], refs[6:]
    vocab_rows, width = w.shape
    block, strip = 512, 128
    lane = lax.broadcasted_iota(jnp.int32, (1, strip), 1)
    start = 0
    for values, id_part in zip(logits, ids):
        at = pl.ds(start, values.shape[0])
        hits = id_part[...] - here[4]
        for k in range(0, vocab_rows, strip):
            onehot = (hits - k == lane).astype(F32)
            errors[at, k : k + strip] = (
                jnp.exp(values[:, k : k + strip] - log_total[at, :]) - onehot
            ).astype(BF16)
        start += values.shape[0]

    places = []
    unit = keep.shape[0] // 4
    start = 0
    for other, a, first, count in PARTS:
        rows = unit * count // 4
        places.append((send if other else keep, a * unit + unit * first // 4, start, rows))
        start += rows

    def step(j, _):
        cols = pl.ds(pl.multiple_of(j * block, block), block)
        grad = (jnp.dot(errors[...], w[:, cols], preferred_element_type=F32) * (width ** (-0.5))).astype(BF16)
        for out, to, start, rows in places:
            out[to : to + rows, cols] = grad[start : start + rows]
        return 0

    lax.fori_loop(0, width // block, step, 0)


def outer_kernel(here, outer, momentum, w0, w1, w2, w3, g0, g1, g2, new_outer, new_momentum, rounded):
    mean_weight = (to_f32(w0[...]) + to_f32(w1[...]) + to_f32(w2[...]) + to_f32(w3[...])) / 4
    slab_grad = g0[...] + to_f32(g1[...]) + to_f32(g2[...])
    pseudo_grad = outer[...] - (mean_weight - (inner_rate / 4) * slab_grad)
    moved = momentum_coef * momentum[...] + pseudo_grad
    new_momentum[...] = moved
    out = outer[...] - outer_rate * (pseudo_grad + momentum_coef * moved)
    new_outer[...] = out
    rounded[...] = out.astype(BF16)


def place_kernel(part, here, first, *refs):
    pieces, out = (first, *refs[:-1]), refs[-1]
    mine, up, low, high, down = pieces
    half = low.shape[0]
    at = lambda k: pl.ds(pl.multiple_of(lax.rem(here[5] + k, 4) * part, part), part)
    out[:, at(0)] = mine[...]
    out[:, at(1)] = up[...]
    out[:half, at(2)] = low[...]
    out[half:, at(2)] = high[...]
    out[:, at(3)] = down[...]


def per_device(hidden, targets, unembed, outer_weight, momentum):
    weights = unembed[0]
    vocab_rows, width = weights.shape
    own = hidden.shape[1]
    slab_rows, part = outer_weight.shape
    reps = lax.axis_size("rep")
    rep = lax.axis_index("rep")
    tokens = own * lax.axis_size(TOK_VOC)
    group_index = lax.axis_index(TOK) * lax.axis_size(VOC) + lax.axis_index(VOC)
    here = jnp.stack(
        [lax.axis_index(a) for a in TOK_VOC] + [group_index * vocab_rows, rep]
    ).astype(jnp.int32)

    ids = targets[0]
    codes = jnp.stack((ids >> 8, ids & 255), 1).astype(BF16)
    piece = jnp.concatenate((hidden[0], jnp.pad(codes, ((0, 0), (0, 126)))), 1)
    across = take(piece, Z, 1)
    piece = jnp.concatenate((piece, across))
    line = jnp.concatenate((piece, take_inner(piece, 1), take_inner(piece, 2), take_inner(piece, -1)))
    up = take_outer(line, 1)
    down = take_outer(line, -1)
    cut = line.shape[0] // 2
    far_up = take_outer(up[:cut], 1)
    far_down = take_outer(down[cut:], -1)

    def with_other(*parts):
        return (*parts, *[take(one, CORE, 1) for one in parts])

    def features(value, k):
        return lax.dynamic_slice_in_dim(value, ((rep + k) % reps) * part, part, 1)

    slab = weights[:slab_rows]
    slab_weights = [features(slab, 0)]
    for k in (1, 2, 3):
        slab_weights.append(take(features(slab, -k), "rep", k))

    def logits_of(parts, w, tables):
        rows = sum(one.shape[0] for one in parts)
        out = [
            shaped(F32, rows, vocab_rows),
            shaped(jnp.int32, rows, 1),
            shaped(BF16, rows, width),
            shaped(F32, *((8, tokens) if len(tables) == 2 else (rows, 128))),
        ]
        kind = {}
        if not tables:
            out.append(shaped(BF16, vocab_rows, width))
            kind = dict(
                scratch=[pltpu.SemaphoreType.DMA((4,))],
                specs={len(parts) + 1: pl.BlockSpec(memory_space=pltpu.HBM)},
            )
        return call(
            functools.partial(logits_kernel, own, len(parts), len(tables)),
            out, here, *parts, w, *tables,
            flops=2 * max(rows, 256) * vocab_rows * width, **kind,
        )

    logits_0, ids_0, states_0, table_0, w = logits_of(with_other(line), weights, ())
    logits_1, ids_1, states_1, table_1 = logits_of(with_other(up, down), w, (table_0,))
    logits_2, ids_2, states_2, stats = logits_of(with_other(far_up, far_down), w, (table_0, table_1))
    logits, every_id = (logits_0, logits_1, logits_2), (ids_0, ids_1, ids_2)
    states = (states_0, states_1, states_2)

    def ring_stats(value, axis):
        return [value] + [take(value, axis, k) for k in (1, 2, 3)]

    stats = lax.all_gather(stats, TOK)
    stats = call(merge_kernel, shaped(F32, 8, tokens), here, stats)
    stats = call(merge_kernel, shaped(F32, 8, tokens), here, *ring_stats(stats, X))
    stats = ring_stats(stats, Y)

    half = slab_rows // 2
    loss, log_total, *grads = call(
        functools.partial(slab_kernel, own, part),
        (
            shaped(F32, own, 1),
            shaped(F32, tokens, 1),
            shaped(F32, slab_rows, part),
            shaped(BF16, slab_rows, part),
            shaped(BF16, half, part),
            shaped(BF16, half, part),
            shaped(BF16, slab_rows, part),
        ),
        here, *stats, *logits, *every_id, *states,
        flops=2 * tokens * slab_rows * width,
        scratch=[pltpu.VMEM((tokens, slab_rows), BF16)],
    )
    token_loss = loss.reshape(1, own)

    keep, send = call(
        hidden_kernel,
        (shaped(BF16, tokens // 2, width), shaped(BF16, tokens // 2, width)),
        here, *logits, *every_id, log_total, w,
        flops=2 * tokens * vocab_rows * width,
        scratch=[pltpu.VMEM((tokens, vocab_rows), BF16)],
    )

    slab_grads = ring_reduce(grads, along("rep"))
    new_outer, new_momentum, rounded = call(
        outer_kernel,
        (shaped(F32, slab_rows, part), shaped(F32, slab_rows, part), shaped(BF16, slab_rows, part)),
        here, outer_weight, momentum, *slab_weights, *slab_grads,
    )
    pieces = ring_gather(rounded, along("rep"))
    next_inner = call(
        functools.partial(place_kernel, part), shaped(BF16, slab_rows, width), here, *pieces
    )

    total = (to_f32(keep) + to_f32(take(send, CORE, 1))).reshape(4, 8 * own, width)
    rounded = total.astype(BF16)
    parts = (total[0], total[1], rounded[2, : 4 * own], rounded[2, 4 * own :], total[3])
    here_part, *got = ring_reduce(parts, take_outer)
    line = (here_part + to_f32(got[0]) + to_f32(got[1])).reshape(4, 2 * own, width)
    rounded = line.astype(BF16)
    pair = line[0] + sum(to_f32(take_inner(rounded[k], -k)) for k in (1, 2, 3))
    token_grad = pair[:own] + to_f32(take(pair[own:].astype(BF16), Z, 1))
    return (token_loss, token_grad[None], new_outer, new_momentum, next_inner)


def solution(mesh):
    finer = Mesh(
        mesh.devices.reshape(mesh.shape["rep"], 2, 2, 4, 4),
        ("rep", "tok_0", "tok_1", "voc_0", "voc_1"),
    )
    in_specs = (
        P("rep", TOK_VOC, None),
        P("rep", TOK_VOC),
        P("rep", TOK_VOC, None),
        P(TOK_VOC, "rep"),
        P(TOK_VOC, "rep"),
    )
    out_specs = (
        P("rep", TOK_VOC),
        P("rep", TOK_VOC, None),
        P(TOK_VOC, "rep"),
        P(TOK_VOC, "rep"),
        P(TOK_VOC, None),
    )

    return jax.shard_map(per_device, mesh=finer, in_specs=in_specs, out_specs=out_specs, check_vma=False)
```

```python
import functools

import jax
import jax.numpy as jnp
from jax import lax
from jax.experimental import pallas as pl
from jax.experimental.pallas import tpu as pltpu
from jax.sharding import Mesh
from jax.sharding import PartitionSpec as P

TOK = ("tok_0", "tok_1")
VOC = ("voc_0", "voc_1")
TOK_VOC = ("tok_0", "tok_1", "voc_0", "voc_1")
Z, CORE, X, Y = TOK_VOC
F32, BF16 = jnp.float32, jnp.bfloat16

PARTS = (
    (0, 0, 0, 4), (1, 0, 0, 4),
    (0, 1, 0, 4), (0, 3, 0, 4), (1, 1, 0, 4), (1, 3, 0, 4),
    (0, 2, 0, 2), (0, 2, 2, 2), (1, 2, 0, 2), (1, 2, 2, 2),
)


inner_rate = 0.5
outer_rate = 0.7
momentum_coef = 0.9
SMEM = pl.BlockSpec(memory_space=pltpu.SMEM)
VMEM = pl.BlockSpec(memory_space=pltpu.VMEM)


def call(kernel, out, *operands, flops=0, scratch=(), limit=16, specs={}, out_spec=VMEM):
    moved = sum(leaf.size * leaf.dtype.itemsize for leaf in jax.tree.leaves((operands, out)))
    return pl.pallas_call(
        kernel,
        in_specs=[SMEM] + [specs.get(k, VMEM) for k in range(1, len(operands))],
        out_specs=jax.tree.map(lambda _: out_spec, out),
        out_shape=out,
        scratch_shapes=scratch,
        compiler_params=pltpu.CompilerParams(vmem_limit_bytes=limit << 20),
        cost_estimate=pl.CostEstimate(
            flops=flops or moved, bytes_accessed=moved, transcendentals=0
        ),
    )(*operands)


def shaped(dtype, *shape):
    return jax.ShapeDtypeStruct(shape, dtype)


def by_core(k, inner):
    pairs = []
    for core in range(2):
        for x in range(4):
            for y in range(4):
                along_x = (core == 1) != inner
                fx, fy = ((x + k) % 4, y) if along_x else (x, (y + k) % 4)
                pairs.append(((core * 4 + fx) * 4 + fy, (core * 4 + x) * 4 + y))
    return pairs


def take_outer(value, k):
    return lax.ppermute(value, (CORE, X, Y), by_core(k, False))


def take_inner(value, k):
    return lax.ppermute(value, (CORE, X, Y), by_core(k, True))


def take_across(value, k):
    pairs = by_core(k, True)
    half = len(pairs)
    both = [(a + (1 - z) * half, b + z * half) for z in range(2) for a, b in pairs]
    return lax.ppermute(value, (Z, CORE, X, Y), both)


def take(value, axis, k):
    n = lax.axis_size(axis)
    return lax.ppermute(value, axis, [((i + k) % n, i) for i in range(n)])


def along(axis):
    return lambda value, k: take(value, axis, k)


def ring_gather(value, take):
    half = value.shape[0] // 2
    up = take(value, 1)
    down = take(value, -1)
    far_up = take(up[:half], 1)
    far_down = take(down[half:], -1)
    return value, up, far_up, far_down, down


def to_f32(value):
    return value.astype(F32)


def arrivals(pieces, take):
    found = []
    for k, piece in zip((2, 1, 3), (pieces[1], pieces[0], pieces[2])):
        found.append(take(piece, -k))
    return found


def part_tokens(here, own, other, a, first, count):
    row = lax.broadcasted_iota(jnp.int32, (count * 2 * own, 1), 0)
    t, plane, b = row % own, row // own % 2, row // (2 * own) + first
    z, c = (here[0] + plane) % 2, (here[1] + other) % 2
    x = (here[2] + jnp.where(c == 0, b, a)) % 4
    y = (here[3] + jnp.where(c == 0, a, b)) % 4
    return (((z * 2 + c) * 4 + x) * 4 + y) * own + t


def token_table(here, tokens, own):
    lane = lax.broadcasted_iota(jnp.int32, (1, tokens), 1)
    rows = [
        part_tokens(here, own, other, a, first, count) == lane for other, a, first, count in PARTS
    ]
    return jnp.concatenate([one.astype(F32) for one in rows]).astype(BF16)


def in_three(value):
    high = value.astype(BF16)
    rest = value - high.astype(F32)
    middle = rest.astype(BF16)
    return high, middle, (rest - middle.astype(F32)).astype(BF16)


def reordered(value, table, dims):
    dot = lambda one: lax.dot_general(one, table, (dims, ((), ())), preferred_element_type=F32)
    return sum(dot(one) for one in in_three(value))


def logits_kernel(count, before, here, *refs):
    parts, refs = refs[:count], refs[count:]
    first = not before
    w_in, tables, (logits, ids, states, table, *more) = refs[0], refs[1 : 1 + before], refs[1 + before :]
    w = more[0] if first else w_in
    vocab_rows, width = w.shape
    block = 256

    def copy(k):
        at = pl.ds(k * block, block)
        return pltpu.make_async_copy(w_in.at[at, :], w.at[at, :], more[1].at[k])

    if first:
        for k in range(vocab_rows // block):
            copy(k).start()
    start = 0
    for part in parts:
        at = pl.ds(start, part.shape[0])
        states[at, :] = part[:, :width]
        codes = part[:, width:].astype(F32).astype(jnp.int32)
        ids[at, :] = codes[:, :1] * 256 + codes[:, 1:2]
        start += part.shape[0]
    rows = states.shape[0]
    lane = lax.broadcasted_iota(jnp.int32, (1, 128), 1)

    def step(j, carry):
        top, total, target = carry
        column = pl.multiple_of(j * block, block)
        if first:
            rows_at = pl.ds(column, block)
            pltpu.make_async_copy(w_in.at[rows_at, :], w.at[rows_at, :], more[1].at[j]).wait()
        out = lax.dot_general(
            states[...], w[pl.ds(column, block), :], (((1,), (1,)), ((), ())),
            preferred_element_type=F32,
        ) * (width ** (-0.5))
        logits[:, pl.ds(column, block)] = out
        hits = ids[...] - (here[4] + column)
        lanes = [out[:, k : k + 128] for k in range(0, block, 128)]
        peak = top
        for one in lanes:
            peak = jnp.maximum(peak, one)
        total = total * jnp.exp(top - peak)
        for k, one in enumerate(lanes):
            total = total + jnp.exp(one - peak)
            target = target + jnp.where(hits - k * 128 == lane, one, 0.0)
        return peak, total, target

    zero = jnp.zeros((rows, 128), F32)
    peak, total, target = lax.fori_loop(
        0, vocab_rows // block, step, (jnp.full((rows, 128), -jnp.inf, F32), zero, zero)
    )
    best = jnp.max(peak, axis=1, keepdims=True)
    mass = jnp.sum(total * jnp.exp(peak - best), axis=1, keepdims=True)
    hit = jnp.sum(target, axis=1, keepdims=True)
    mine = jnp.where(lane == 0, best, jnp.where(lane == 1, mass, jnp.where(lane == 2, hit, 0.0)))
    if before < 3:
        table[...] = mine
    else:
        every = jnp.concatenate([one[...] for one in tables[:2]] + [mine])
        table[...] = reordered(every, tables[2][...], ((0,), (0,)))[:8]


def merged(parts):
    top = parts[0][0:1]
    for one in parts[1:]:
        top = jnp.maximum(top, one[0:1])
    total = sum(one[1:2] * jnp.exp(one[0:1] - top) for one in parts)
    return top, total, sum(one[2:3] for one in parts)


def merge_kernel(here, got, out):
    top, total, target = merged([got[k] for k in range(got.shape[0])])
    row = lax.broadcasted_iota(jnp.int32, out.shape[1:], 0)
    stats = jnp.where(row == 0, top, jnp.where(row == 1, total, jnp.where(row == 2, target, 0.0)))
    for k in range(out.shape[0]):
        out[k] = stats


def slab_kernel(own, part, here, *refs):
    got, logits, ids, states, table, outs = refs[0], refs[1:4], refs[4:7], refs[7:10], refs[10], refs[11:]
    loss, log_total, mine, *sent, errors = outs
    width = 4 * part
    top, total, target = merged([got[k] for k in range(got.shape[0])])
    every = top + jnp.log(total)
    row = lax.broadcasted_iota(jnp.int32, got.shape[1:], 0)
    both = jnp.where(row == 0, every, jnp.where(row == 1, every - target, 0.0))
    columns = sum(
        lax.dot_general(table[...], one, (((1,), (1,)), ((), ())), preferred_element_type=F32)
        for one in in_three(both)
    )
    log_total[...] = columns[:, 0:1]
    loss[...] = columns[:own, 1:2]
    strip = mine.shape[0]
    lane = lax.broadcasted_iota(jnp.int32, (1, strip), 1)
    start = 0
    for values, id_part in zip(logits, ids):
        end = start + values.shape[0]
        onehot = (id_part[...] - here[4] == lane).astype(F32)
        part_errors = jnp.exp(values[:, :strip] - columns[start:end, 0:1]) - onehot
        errors[:, start:end] = part_errors.T.astype(BF16)
        start = end

    def grad(k):
        at = pl.multiple_of(lax.rem(here[5] + k, 4) * part, part)
        total, start = 0.0, 0
        for state in states:
            end = start + state.shape[0]
            total += jnp.dot(
                errors[:, start:end], state[:, pl.ds(at, part)], preferred_element_type=F32
            )
            start = end
        return total * (width ** (-0.5))

    for k in (2, 1, 3):
        sent[k - 1][...] = grad(k).astype(BF16)
    mine[...] = grad(0)


def hidden_kernel(other, here, *refs):
    logits, ids, (log_total, w, out, errors) = refs[:3], refs[3:6], refs[6:]
    vocab_rows, width = w.shape
    block, strip = 512, 128
    lane = lax.broadcasted_iota(jnp.int32, (1, strip), 1)
    unit = out.shape[0] // 4
    start = 0
    for values, id_part, lines in zip(logits, ids, ((0,), (1, 3), (2,))):
        for n, line in enumerate(lines):
            first = (other * len(lines) + n) * unit
            hits = id_part[first : first + unit, :] - here[4]
            total = log_total[start + first : start + first + unit, :]
            for k in range(0, vocab_rows, strip):
                onehot = (hits - k == lane).astype(F32)
                errors[line * unit : (line + 1) * unit, k : k + strip] = (
                    jnp.exp(values[first : first + unit, k : k + strip] - total) - onehot
                ).astype(BF16)
        start += values.shape[0]

    def step(j, _):
        cols = pl.ds(pl.multiple_of(j * block, block), block)
        grad = jnp.dot(errors[...], w[:, cols], preferred_element_type=F32) * (width ** (-0.5))
        out[:, cols] = grad.astype(BF16)
        return 0

    lax.fori_loop(0, width // block, step, 0)


def outer_kernel(here, outer, momentum, w0, w1, w2, w3, g0, g1, g2, g3, *outs):
    mean_weight = (to_f32(w0[...]) + to_f32(w1[...]) + to_f32(w2[...]) + to_f32(w3[...])) / 4
    slab_grad = g0[...] + to_f32(g1[...]) + to_f32(g2[...]) + to_f32(g3[...])
    pseudo_grad = outer[...] - (mean_weight - (inner_rate / 4) * slab_grad)
    moved = momentum_coef * momentum[...] + pseudo_grad
    new_outer = outer[...] - outer_rate * (pseudo_grad + momentum_coef * moved)
    outs[0][...] = new_outer.astype(outs[0].dtype)
    if len(outs) == 2:
        outs[1][...] = moved


def join_kernel(here, *refs):
    pieces, out = refs[:-1], refs[-1]
    rows = pieces[0].shape[0]
    for k, piece in enumerate(pieces):
        out[k * rows : (k + 1) * rows, :] = piece[...]


def table_kernel(own, here, out):
    out[...] = token_table(here, out.shape[0], own)


def loss_kernel(here, column, row):
    size = column.shape[0]
    at = [lax.broadcasted_iota(jnp.int32, (size, size), dim) for dim in (0, 1)]
    row[...] = jnp.sum(jnp.where(at[0] == at[1], column[...], 0.0), axis=0, keepdims=True)


def place_kernel(part, here, mine, up, low, high, down, out, sems):
    half = low.shape[0]

    def copy(piece, k, first, n):
        at = pl.multiple_of(lax.rem(here[5] + k, 4) * part, part)
        to = out.at[pl.ds(first, piece.shape[0]), pl.ds(at, part)]
        return pltpu.make_async_copy(piece, to, sems.at[n])

    copies = [
        copy(mine, 0, 0, 0), copy(up, 1, 0, 1), copy(low, 2, 0, 2), copy(high, 2, half, 3), copy(down, 3, 0, 4)
    ]
    for one in copies:
        one.start()
    for one in copies:
        one.wait()


def per_device(hidden, targets, unembed, outer_weight, momentum):
    weights = unembed[0]
    vocab_rows, width = weights.shape
    own = hidden.shape[1]
    slab_rows, part = outer_weight.shape
    reps = lax.axis_size("rep")
    rep = lax.axis_index("rep")
    tokens = own * lax.axis_size(TOK_VOC)
    group_index = lax.axis_index(TOK) * lax.axis_size(VOC) + lax.axis_index(VOC)
    here = jnp.stack(
        [lax.axis_index(a) for a in TOK_VOC] + [group_index * vocab_rows, rep]
    ).astype(jnp.int32)

    ids = targets[0]
    codes = jnp.stack((ids >> 8, ids & 255), 1).astype(BF16)
    piece = jnp.concatenate((hidden[0], jnp.pad(codes, ((0, 0), (0, 126)))), 1)
    cells = {(0, 0): piece}
    order = call(functools.partial(table_kernel, own), shaped(BF16, tokens, tokens), here)
    for k in (2, 1, 3, 0):
        for plane, get in ((1, take_across), (0, take_inner)):
            if k or plane:
                cells[k, plane] = get(piece, k)
    cells = [cells[k, plane] for k in range(4) for plane in range(2)]
    line = call(join_kernel, shaped(BF16, 8 * own, piece.shape[1]), here, *cells)
    up = take_outer(line, 1)
    down = take_outer(line, -1)
    cut = line.shape[0] // 2
    far_up = take_outer(up[:cut], 1)
    far_down = take_outer(down[cut:], -1)

    def with_other(*parts):
        return (*parts, *[take(one, CORE, 1) for one in parts])

    def features(value, k):
        return lax.dynamic_slice_in_dim(value, ((rep + k) % reps) * part, part, 1)

    slab = weights[:slab_rows]
    slab_weights = [features(slab, 0)]
    for k in (1, 2, 3):
        slab_weights.append(take(features(slab, -k), "rep", k))

    def logits_of(parts, w, tables):
        rows = sum(one.shape[0] for one in parts)
        out = [
            shaped(F32, rows, vocab_rows),
            shaped(jnp.int32, rows, 1),
            shaped(BF16, rows, width),
            shaped(F32, *((8, tokens) if len(tables) == 3 else (rows, 128))),
        ]
        kind = {}
        if not tables:
            out.append(shaped(BF16, vocab_rows, width))
            kind = dict(
                scratch=[pltpu.SemaphoreType.DMA((4,))],
                specs={len(parts) + 1: pl.BlockSpec(memory_space=pltpu.HBM)},
                limit=40,
            )
        return call(
            functools.partial(logits_kernel, len(parts), len(tables)),
            out, here, *parts, w, *tables,
            flops=2 * max(rows, 256) * vocab_rows * width, **kind,
        )

    logits_0, ids_0, states_0, table_0, w = logits_of(with_other(line), weights, ())
    logits_1, ids_1, states_1, table_1 = logits_of(with_other(up, down), w, (table_0,))
    logits_2, ids_2, states_2, stats = logits_of(with_other(far_up, far_down), w, (table_0, table_1, order))
    logits, every_id = (logits_0, logits_1, logits_2), (ids_0, ids_1, ids_2)
    states = (states_0, states_1, states_2)

    stats = lax.all_gather(stats, TOK)
    stats = call(merge_kernel, shaped(F32, lax.axis_size(VOC), 4, tokens), here, stats)
    stats = lax.all_to_all(stats, VOC, 0, 0, tiled=True)

    loss, log_total, mine, *grads = call(
        functools.partial(slab_kernel, own, part),
        (
            shaped(F32, own, 1),
            shaped(F32, tokens, 1),
            shaped(F32, slab_rows, part),
            *[shaped(BF16, slab_rows, part)] * 3,
        ),
        here, stats, *logits, *every_id, *states, order,
        flops=2 * tokens * slab_rows * width,
        scratch=[pltpu.VMEM((slab_rows, tokens), BF16)],
    )
    token_loss = call(loss_kernel, shaped(F32, 1, own), here, loss)

    def hidden_terms(other):
        return call(
            functools.partial(hidden_kernel, other), shaped(BF16, tokens // 2, width),
            here, *logits, *every_id, log_total, w,
            flops=tokens * vocab_rows * width,
            scratch=[pltpu.VMEM((tokens // 2, vocab_rows), BF16)],
        )

    send = hidden_terms(1)
    keep = hidden_terms(0)

    slab_grads = [mine, *arrivals(grads, along("rep"))]
    operands = (here, outer_weight, momentum, *slab_weights, *slab_grads)
    rounded = call(outer_kernel, shaped(BF16, slab_rows, part), *operands)
    new_outer, new_momentum = call(outer_kernel, [shaped(F32, slab_rows, part)] * 2, *operands)
    pieces = ring_gather(rounded, along("rep"))
    next_inner = call(
        functools.partial(place_kernel, part), shaped(BF16, slab_rows, width), here, *pieces,
        scratch=[pltpu.SemaphoreType.DMA((5,))], out_spec=pl.BlockSpec(memory_space=pltpu.HBM),
    )

    got = take(send, CORE, 1)
    total = (to_f32(keep) + to_f32(got)).reshape(4, 8 * own, width)
    rounded = total.astype(BF16)
    got = arrivals(rounded[1:], take_outer)
    line = (total[0] + sum(to_f32(one) for one in got)).reshape(4, 2 * own, width)
    rounded = line.astype(BF16)
    pair = line[0] + sum(to_f32(take_inner(rounded[k], -k)) for k in (1, 2, 3))
    pair_sent = take(pair[own:].astype(BF16), Z, 1)
    token_grad = (pair[:own] + to_f32(pair_sent))[None]
    return (token_loss, token_grad, new_outer, new_momentum, next_inner)


def solution(mesh):
    finer = Mesh(
        mesh.devices.reshape(mesh.shape["rep"], 2, 2, 4, 4),
        ("rep", "tok_0", "tok_1", "voc_0", "voc_1"),
    )
    in_specs = (
        P("rep", TOK_VOC, None),
        P("rep", TOK_VOC),
        P("rep", TOK_VOC, None),
        P(TOK_VOC, "rep"),
        P(TOK_VOC, "rep"),
    )
    out_specs = (
        P("rep", TOK_VOC),
        P("rep", TOK_VOC, None),
        P(TOK_VOC, "rep"),
        P(TOK_VOC, "rep"),
        P(TOK_VOC, None),
    )

    return jax.shard_map(per_device, mesh=finer, in_specs=in_specs, out_specs=out_specs, check_vma=False)
```

```python
import functools

import jax
import jax.numpy as jnp
from jax import lax
from jax.experimental import pallas as pl
from jax.experimental.pallas import tpu as pltpu
from jax.sharding import Mesh
from jax.sharding import PartitionSpec as P

TOK = ("tok_0", "tok_1")
VOC = ("voc_0", "voc_1")
TOK_VOC = ("tok_0", "tok_1", "voc_0", "voc_1")
Z, CORE, X, Y = TOK_VOC
F32, BF16 = jnp.float32, jnp.bfloat16

GROUPS = (
    ((0, 0, 0, 4), (1, 0, 0, 4)),
    ((0, 1, 0, 4), (0, 3, 0, 4), (1, 1, 0, 4)),
    ((1, 3, 0, 4), (0, 2, 0, 2), (0, 2, 2, 2), (1, 2, 0, 2), (1, 2, 2, 2)),
)
PARTS = sum(GROUPS, ())


inner_rate = 0.5
outer_rate = 0.7
momentum_coef = 0.9
SMEM = pl.BlockSpec(memory_space=pltpu.SMEM)
VMEM = pl.BlockSpec(memory_space=pltpu.VMEM)


def call(kernel, out, *operands, flops=0, scratch=(), limit=16, specs={}, out_spec=VMEM):
    moved = sum(leaf.size * leaf.dtype.itemsize for leaf in jax.tree.leaves((operands, out)))
    return pl.pallas_call(
        kernel,
        in_specs=[SMEM] + [specs.get(k, VMEM) for k in range(1, len(operands))],
        out_specs=jax.tree.map(lambda _: out_spec, out),
        out_shape=out,
        scratch_shapes=scratch,
        compiler_params=pltpu.CompilerParams(vmem_limit_bytes=limit << 20),
        cost_estimate=pl.CostEstimate(
            flops=flops or moved, bytes_accessed=moved, transcendentals=0
        ),
    )(*operands)


def shaped(dtype, *shape):
    return jax.ShapeDtypeStruct(shape, dtype)


def by_core(k, inner):
    pairs = []
    for core in range(2):
        for x in range(4):
            for y in range(4):
                along_x = (core == 1) != inner
                fx, fy = ((x + k) % 4, y) if along_x else (x, (y + k) % 4)
                pairs.append(((core * 4 + fx) * 4 + fy, (core * 4 + x) * 4 + y))
    return pairs


def take_outer(value, k):
    return lax.ppermute(value, (CORE, X, Y), by_core(k, False))


def take_inner(value, k):
    return lax.ppermute(value, (CORE, X, Y), by_core(k, True))


def take(value, axis, k):
    n = lax.axis_size(axis)
    return lax.ppermute(value, axis, [((i + k) % n, i) for i in range(n)])


def along(axis):
    return lambda value, k: take(value, axis, k)


def ring_gather(first, second, take):
    got = {}
    for name, value, k in (
        ("first_up", first, 1), ("first_down", second, -1), ("second_up", second, 1), ("second_down", first, -1)
    ):
        got[name] = take(value, k)
    far_up = take(got["first_up"], 1)
    far_down = take(got["first_down"], -1)
    return (
        first, second, got["first_up"], got["second_up"], far_up, far_down, got["second_down"], got["first_down"]
    )


def to_f32(value):
    return value.astype(F32)


def arrivals(pieces, take):
    found = []
    for k, piece in zip((2, 1, 3), (pieces[1], pieces[0], pieces[2])):
        found.append(take(piece, -k))
    return found


def part_tokens(here, own, other, a, first, count):
    row = lax.broadcasted_iota(jnp.int32, (count * 2 * own, 1), 0)
    t, plane, b = row % own, row // own % 2, row // (2 * own) + first
    z, c = (here[0] + plane) % 2, (here[1] + other) % 2
    x = (here[2] + jnp.where(c == 0, b, a)) % 4
    y = (here[3] + jnp.where(c == 0, a, b)) % 4
    return (((z * 2 + c) * 4 + x) * 4 + y) * own + t


def token_table(here, tokens, own):
    lane = lax.broadcasted_iota(jnp.int32, (1, tokens), 1)
    rows = [
        part_tokens(here, own, other, a, first, count) == lane for other, a, first, count in PARTS
    ]
    return jnp.concatenate([one.astype(F32) for one in rows]).astype(BF16)


def in_three(value):
    high = value.astype(BF16)
    rest = value - high.astype(F32)
    middle = rest.astype(BF16)
    return high, middle, (rest - middle.astype(F32)).astype(BF16)


def reordered(value, table, dims):
    dot = lambda one: lax.dot_general(one, table, (dims, ((), ())), preferred_element_type=F32)
    return sum(dot(one) for one in in_three(value))


def logits_kernel(count, before, here, *refs):
    parts, refs = refs[:count], refs[count:]
    first = not before
    w_in, tables, (logits, ids, states, table, *more) = refs[0], refs[1 : 1 + before], refs[1 + before :]
    w = more[0] if first else w_in
    vocab_rows, width = w.shape
    block = 256

    def copy(k):
        at = pl.ds(k * block, block)
        return pltpu.make_async_copy(w_in.at[at, :], w.at[at, :], more[1].at[k])

    if first:
        for k in range(vocab_rows // block):
            copy(k).start()
    start = 0
    for part in parts:
        at = pl.ds(start, part.shape[0])
        states[at, :] = part[:, :width]
        codes = part[:, width:].astype(F32).astype(jnp.int32)
        ids[at, :] = codes[:, :1] * 256 + codes[:, 1:2]
        start += part.shape[0]
    rows = states.shape[0]
    lane = lax.broadcasted_iota(jnp.int32, (1, 128), 1)

    def step(j, carry):
        top, total, target = carry
        column = pl.multiple_of(j * block, block)
        if first:
            rows_at = pl.ds(column, block)
            pltpu.make_async_copy(w_in.at[rows_at, :], w.at[rows_at, :], more[1].at[j]).wait()
        out = lax.dot_general(
            states[...], w[pl.ds(column, block), :], (((1,), (1,)), ((), ())),
            preferred_element_type=F32,
        ) * (width ** (-0.5))
        logits[:, pl.ds(column, block)] = out
        hits = ids[...] - (here[4] + column)
        lanes = [out[:, k : k + 128] for k in range(0, block, 128)]
        peak = top
        for one in lanes:
            peak = jnp.maximum(peak, one)
        total = total * jnp.exp(top - peak)
        for k, one in enumerate(lanes):
            total = total + jnp.exp(one - peak)
            target = target + jnp.where(hits - k * 128 == lane, one, 0.0)
        return peak, total, target

    zero = jnp.zeros((rows, 128), F32)
    peak, total, target = lax.fori_loop(
        0, vocab_rows // block, step, (jnp.full((rows, 128), -jnp.inf, F32), zero, zero)
    )
    best = jnp.max(peak, axis=1, keepdims=True)
    mass = jnp.sum(total * jnp.exp(peak - best), axis=1, keepdims=True)
    hit = jnp.sum(target, axis=1, keepdims=True)
    mine = jnp.where(lane == 0, best, jnp.where(lane == 1, mass, jnp.where(lane == 2, hit, 0.0)))
    if before < 3:
        table[...] = mine
    else:
        every = jnp.concatenate([one[...] for one in tables[:2]] + [mine])
        table[...] = reordered(every, tables[2][...], ((0,), (0,)))[:8]


def merged(parts):
    top = parts[0][0:1]
    for one in parts[1:]:
        top = jnp.maximum(top, one[0:1])
    total = sum(one[1:2] * jnp.exp(one[0:1] - top) for one in parts)
    return top, total, sum(one[2:3] for one in parts)


def merge_kernel(here, got, out):
    top, total, target = merged([got[k] for k in range(got.shape[0])])
    row = lax.broadcasted_iota(jnp.int32, out.shape[1:], 0)
    stats = jnp.where(row == 0, top, jnp.where(row == 1, total, jnp.where(row == 2, target, 0.0)))
    for k in range(out.shape[0]):
        out[k] = stats


def slab_kernel(own, part, here, *refs):
    got, logits, ids, states, table, outs = refs[0], refs[1:4], refs[4:7], refs[7:10], refs[10], refs[11:]
    loss, log_total, mine, *sent, errors = outs
    width = 4 * part
    top, total, target = merged([got[k] for k in range(got.shape[0])])
    every = top + jnp.log(total)
    row = lax.broadcasted_iota(jnp.int32, got.shape[1:], 0)
    both = jnp.where(row == 0, every, jnp.where(row == 1, every - target, 0.0))
    columns = sum(
        lax.dot_general(table[...], one, (((1,), (1,)), ((), ())), preferred_element_type=F32)
        for one in in_three(both)
    )
    log_total[...] = columns[:, 0:1]
    loss[...] = columns[:own, 1:2]
    strip = mine.shape[0]
    lane = lax.broadcasted_iota(jnp.int32, (1, strip), 1)
    start = 0
    for values, id_part in zip(logits, ids):
        end = start + values.shape[0]
        onehot = (id_part[...] - here[4] == lane).astype(F32)
        part_errors = jnp.exp(values[:, :strip] - columns[start:end, 0:1]) - onehot
        errors[:, start:end] = part_errors.T.astype(BF16)
        start = end

    def grad(k):
        at = pl.multiple_of(lax.rem(here[5] + k, 4) * part, part)
        total, start = 0.0, 0
        for state in states:
            end = start + state.shape[0]
            total += jnp.dot(
                errors[:, start:end], state[:, pl.ds(at, part)], preferred_element_type=F32
            )
            start = end
        return total * (width ** (-0.5))

    for k in (2, 1, 3):
        sent[k - 1][...] = grad(k).astype(BF16)
    mine[...] = grad(0)


def hidden_kernel(other, here, *refs):
    logits, ids, (log_total, w, out, errors) = refs[:3], refs[3:6], refs[6:]
    vocab_rows, width = w.shape
    block, strip = 512, 128
    lane = lax.broadcasted_iota(jnp.int32, (1, strip), 1)
    unit = out.shape[0] // 4
    start = 0
    for values, id_part, parts in zip(logits, ids, GROUPS):
        first = 0
        for whose, line, cell, count in parts:
            last = first + unit * count // 4
            to = line * unit + unit * cell // 4
            if whose == other:
                hits = id_part[first:last, :] - here[4]
                total = log_total[start + first : start + last, :]
                for k in range(0, vocab_rows, strip):
                    onehot = (hits - k == lane).astype(F32)
                    errors[to : to + last - first, k : k + strip] = (
                        jnp.exp(values[first:last, k : k + strip] - total) - onehot
                    ).astype(BF16)
            first = last
        start += first

    def step(j, _):
        cols = pl.ds(pl.multiple_of(j * block, block), block)
        grad = jnp.dot(errors[...], w[:, cols], preferred_element_type=F32) * (width ** (-0.5))
        out[:, cols] = grad.astype(BF16)
        return 0

    lax.fori_loop(0, width // block, step, 0)


def outer_kernel(here, outer, momentum, w0, w1, w2, w3, g0, g1, g2, g3, *outs):
    mean_weight = (to_f32(w0[...]) + to_f32(w1[...]) + to_f32(w2[...]) + to_f32(w3[...])) / 4
    slab_grad = g0[...] + to_f32(g1[...]) + to_f32(g2[...]) + to_f32(g3[...])
    pseudo_grad = outer[...] - (mean_weight - (inner_rate / 4) * slab_grad)
    moved = momentum_coef * momentum[...] + pseudo_grad
    new_outer = outer[...] - outer_rate * (pseudo_grad + momentum_coef * moved)
    if outs[0].dtype == F32:
        outs[0][...], outs[1][...] = new_outer, moved
    else:
        half = outs[0].shape[0]
        outs[0][...], outs[1][...] = new_outer[:half].astype(BF16), new_outer[half:].astype(BF16)


def grad_kernel(here, first, second, third, fourth, *outs):
    rows = outs[0].shape[0]
    for k, out in enumerate(outs):
        at = pl.ds(k * rows, rows)
        value = first[at, :] + to_f32(second[at, :]) + to_f32(third[at, :]) + to_f32(fourth[at, :])
        out[...] = value.astype(out.dtype)


def join_kernel(here, *refs):
    pieces, out = refs[:-1], refs[-1]
    rows = pieces[0].shape[0]
    for k, piece in enumerate(pieces):
        out[k * rows : (k + 1) * rows, :] = piece[...]


def table_kernel(own, here, out):
    out[...] = token_table(here, out.shape[0], own)


def loss_kernel(here, column, row):
    size = column.shape[0]
    at = [lax.broadcasted_iota(jnp.int32, (size, size), dim) for dim in (0, 1)]
    row[...] = jnp.sum(jnp.where(at[0] == at[1], column[...], 0.0), axis=0, keepdims=True)


def place_kernel(part, here, *refs):
    pieces, out, sems = refs[:8], refs[8], refs[9]
    half = pieces[0].shape[0]
    copies = []
    for k, piece in enumerate(pieces):
        at = pl.multiple_of(lax.rem(here[5] + k // 2, 4) * part, part)
        to = out.at[pl.ds(k % 2 * half, half), pl.ds(at, part)]
        copies.append(pltpu.make_async_copy(piece, to, sems.at[k]))
    for one in copies:
        one.start()
    for one in copies:
        one.wait()


def per_device(hidden, targets, unembed, outer_weight, momentum):
    weights = unembed[0]
    vocab_rows, width = weights.shape
    own = hidden.shape[1]
    slab_rows, part = outer_weight.shape
    reps = lax.axis_size("rep")
    rep = lax.axis_index("rep")
    tokens = own * lax.axis_size(TOK_VOC)
    group_index = lax.axis_index(TOK) * lax.axis_size(VOC) + lax.axis_index(VOC)
    here = jnp.stack(
        [lax.axis_index(a) for a in TOK_VOC] + [group_index * vocab_rows, rep]
    ).astype(jnp.int32)

    ids = targets[0]
    codes = jnp.stack((ids >> 8, ids & 255), 1).astype(BF16)
    piece = jnp.concatenate((hidden[0], jnp.pad(codes, ((0, 0), (0, 126)))), 1)
    across = take(piece, Z, 1)
    piece = call(join_kernel, shaped(BF16, 2 * own, piece.shape[1]), here, piece, across)
    order = call(functools.partial(table_kernel, own), shaped(BF16, tokens, tokens), here)
    inner = {}
    for k in (2, 1, 3):
        inner[k] = take_inner(piece, k)
    line = call(
        join_kernel, shaped(BF16, 8 * own, piece.shape[1]), here, piece, inner[1], inner[2], inner[3]
    )
    up = take_outer(line, 1)
    down = take_outer(line, -1)
    cut = line.shape[0] // 2
    far_up = take_outer(up[:cut], 1)
    far_down = take_outer(down[cut:], -1)

    def swapped(*parts):
        return [take(one, CORE, 1) for one in parts]

    parts_0 = line, *swapped(line)
    up_swapped, down_swapped = swapped(up, down)
    parts_1 = up, down, up_swapped
    parts_2 = down_swapped, far_up, far_down, *swapped(far_up, far_down)

    def features(value, k):
        return lax.dynamic_slice_in_dim(value, ((rep + k) % reps) * part, part, 1)

    slab = weights[:slab_rows]
    slab_weights = [features(slab, 0)]
    for k in (1, 2, 3):
        slab_weights.append(take(features(slab, -k), "rep", k))

    def logits_of(parts, w, tables):
        rows = sum(one.shape[0] for one in parts)
        out = [
            shaped(F32, rows, vocab_rows),
            shaped(jnp.int32, rows, 1),
            shaped(BF16, rows, width),
            shaped(F32, *((8, tokens) if len(tables) == 3 else (rows, 128))),
        ]
        kind = {}
        if not tables:
            out.append(shaped(BF16, vocab_rows, width))
            kind = dict(
                scratch=[pltpu.SemaphoreType.DMA((4,))],
                specs={len(parts) + 1: pl.BlockSpec(memory_space=pltpu.HBM)},
                limit=40,
            )
        return call(
            functools.partial(logits_kernel, len(parts), len(tables)),
            out, here, *parts, w, *tables,
            flops=2 * max(rows, 256) * vocab_rows * width, **kind,
        )

    logits_0, ids_0, states_0, table_0, w = logits_of(parts_0, weights, ())
    logits_1, ids_1, states_1, table_1 = logits_of(parts_1, w, (table_0,))
    logits_2, ids_2, states_2, stats = logits_of(parts_2, w, (table_0, table_1, order))
    logits, every_id = (logits_0, logits_1, logits_2), (ids_0, ids_1, ids_2)
    states = (states_0, states_1, states_2)

    stats = lax.all_gather(stats, TOK)
    stats = call(merge_kernel, shaped(F32, lax.axis_size(VOC), 4, tokens), here, stats)
    stats = lax.all_to_all(stats, VOC, 0, 0, tiled=True)

    loss, log_total, mine, *grads = call(
        functools.partial(slab_kernel, own, part),
        (
            shaped(F32, own, 1),
            shaped(F32, tokens, 1),
            shaped(F32, slab_rows, part),
            *[shaped(BF16, slab_rows, part)] * 3,
        ),
        here, stats, *logits, *every_id, *states, order,
        flops=2 * tokens * slab_rows * width,
        scratch=[pltpu.VMEM((slab_rows, tokens), BF16)],
    )
    token_loss = call(loss_kernel, shaped(F32, 1, own), here, loss)

    def hidden_terms(other):
        return call(
            functools.partial(hidden_kernel, other), shaped(BF16, tokens // 2, width),
            here, *logits, *every_id, log_total, w,
            flops=tokens * vocab_rows * width,
            scratch=[pltpu.VMEM((tokens // 2, vocab_rows), BF16)],
        )

    send = hidden_terms(1)
    keep = hidden_terms(0)

    slab_grads = [mine, *arrivals(grads, along("rep"))]
    operands = (here, outer_weight, momentum, *slab_weights, *slab_grads)
    rounded = call(outer_kernel, [shaped(BF16, slab_rows // 2, part)] * 2, *operands)
    new_outer, new_momentum = call(outer_kernel, [shaped(F32, slab_rows, part)] * 2, *operands)
    pieces = ring_gather(*rounded, along("rep"))
    next_inner = call(
        functools.partial(place_kernel, part), shaped(BF16, slab_rows, width), here, *pieces,
        scratch=[pltpu.SemaphoreType.DMA((8,))], out_spec=pl.BlockSpec(memory_space=pltpu.HBM),
    )

    got = take(send, CORE, 1)
    total = (to_f32(keep) + to_f32(got)).reshape(4, 8 * own, width)
    rounded = total.astype(BF16)
    got = arrivals(rounded[1:], take_outer)
    pair, *others = call(
        grad_kernel,
        [shaped(F32, 2 * own, width)] + [shaped(BF16, 2 * own, width)] * 3,
        here, total[0], *got,
    )
    for k in (2, 1, 3):
        got = take_inner(others[k - 1], -k)
        pair = pair + to_f32(got)
    pair_sent = take(pair[own:].astype(BF16), Z, 1)
    token_grad = (pair[:own] + to_f32(pair_sent))[None]
    return (token_loss, token_grad, new_outer, new_momentum, next_inner)


def solution(mesh):
    finer = Mesh(
        mesh.devices.reshape(mesh.shape["rep"], 2, 2, 4, 4),
        ("rep", "tok_0", "tok_1", "voc_0", "voc_1"),
    )
    in_specs = (
        P("rep", TOK_VOC, None),
        P("rep", TOK_VOC),
        P("rep", TOK_VOC, None),
        P(TOK_VOC, "rep"),
        P(TOK_VOC, "rep"),
    )
    out_specs = (
        P("rep", TOK_VOC),
        P("rep", TOK_VOC, None),
        P(TOK_VOC, "rep"),
        P(TOK_VOC, "rep"),
        P(TOK_VOC, None),
    )

    return jax.shard_map(per_device, mesh=finer, in_specs=in_specs, out_specs=out_specs, check_vma=False)
```

```python
import functools

import jax
import jax.numpy as jnp
from jax import lax
from jax.experimental import pallas as pl
from jax.experimental.pallas import tpu as pltpu
from jax.sharding import Mesh
from jax.sharding import PartitionSpec as P

TOK = ("tok_0", "tok_1")
VOC = ("voc_0", "voc_1")
TOK_VOC = ("tok_0", "tok_1", "voc_0", "voc_1")
Z, CORE, X, Y = TOK_VOC
F32, BF16 = jnp.float32, jnp.bfloat16

GROUPS = (
    ((0, 0, 0, 4), (1, 0, 0, 4)),
    ((0, 1, 0, 4), (0, 3, 0, 4), (1, 1, 0, 4)),
    ((1, 3, 0, 4), (0, 2, 0, 2), (0, 2, 2, 2), (1, 2, 0, 2), (1, 2, 2, 2)),
)
PARTS = sum(GROUPS, ())


inner_rate = 0.5
outer_rate = 0.7
momentum_coef = 0.9
SMEM = pl.BlockSpec(memory_space=pltpu.SMEM)
VMEM = pl.BlockSpec(memory_space=pltpu.VMEM)


def call(kernel, out, *operands, flops=0, scratch=(), limit=16, specs={}, out_spec=VMEM):
    moved = sum(leaf.size * leaf.dtype.itemsize for leaf in jax.tree.leaves((operands, out)))
    return pl.pallas_call(
        kernel,
        in_specs=[SMEM] + [specs.get(k, VMEM) for k in range(1, len(operands))],
        out_specs=out_spec if isinstance(out_spec, list) else jax.tree.map(lambda _: out_spec, out),
        out_shape=out,
        scratch_shapes=scratch,
        compiler_params=pltpu.CompilerParams(vmem_limit_bytes=limit << 20),
        cost_estimate=pl.CostEstimate(
            flops=flops or moved, bytes_accessed=moved, transcendentals=0
        ),
    )(*operands)


def shaped(dtype, *shape):
    return jax.ShapeDtypeStruct(shape, dtype)


def by_core(k, inner):
    pairs = []
    for core in range(2):
        for x in range(4):
            for y in range(4):
                along_x = (core == 1) != inner
                fx, fy = ((x + k) % 4, y) if along_x else (x, (y + k) % 4)
                pairs.append(((core * 4 + fx) * 4 + fy, (core * 4 + x) * 4 + y))
    return pairs


def take_outer(value, k):
    return lax.ppermute(value, (CORE, X, Y), by_core(k, False))


def take_inner(value, k):
    return lax.ppermute(value, (CORE, X, Y), by_core(k, True))


def take(value, axis, k):
    n = lax.axis_size(axis)
    return lax.ppermute(value, axis, [((i + k) % n, i) for i in range(n)])


def along(axis):
    return lambda value, k: take(value, axis, k)


def ring_gather(first, second, take):
    got = {}
    for name, value, k in (
        ("first_up", first, 1), ("first_down", second, -1), ("second_up", second, 1), ("second_down", first, -1)
    ):
        got[name] = take(value, k)
    far_up = take(got["first_up"], 1)
    far_down = take(got["first_down"], -1)
    return (
        first, second, got["first_up"], got["second_up"], far_up, far_down, got["second_down"], got["first_down"]
    )


def to_f32(value):
    return value.astype(F32)


def arrivals(pieces, take):
    found = []
    for k, piece in zip((2, 1, 3), (pieces[1], pieces[0], pieces[2])):
        found.append(take(piece, -k))
    return found


def part_tokens(here, own, other, a, first, count):
    row = lax.broadcasted_iota(jnp.int32, (count * 2 * own, 1), 0)
    t, plane, b = row % own, row // own % 2, row // (2 * own) + first
    z, c = (here[0] + plane) % 2, (here[1] + other) % 2
    x = (here[2] + jnp.where(c == 0, b, a)) % 4
    y = (here[3] + jnp.where(c == 0, a, b)) % 4
    return (((z * 2 + c) * 4 + x) * 4 + y) * own + t


def token_table(here, tokens, own):
    lane = lax.broadcasted_iota(jnp.int32, (1, tokens), 1)
    rows = [
        part_tokens(here, own, other, a, first, count) == lane for other, a, first, count in PARTS
    ]
    return jnp.concatenate([one.astype(F32) for one in rows]).astype(BF16)


def in_three(value):
    high = value.astype(BF16)
    rest = value - high.astype(F32)
    middle = rest.astype(BF16)
    return high, middle, (rest - middle.astype(F32)).astype(BF16)


def reordered(value, table, dims):
    dot = lambda one: lax.dot_general(one, table, (dims, ((), ())), preferred_element_type=F32)
    return sum(dot(one) for one in in_three(value))


def logits_kernel(count, before, here, *refs):
    parts, refs = refs[:count], refs[count:]
    first = not before
    w_in, tables, (logits, ids, states, table, *more) = refs[0], refs[1 : 1 + before], refs[1 + before :]
    w = more[0] if first else w_in
    vocab_rows, width = w.shape
    block = 256

    def copy(k):
        at = pl.ds(k * block, block)
        return pltpu.make_async_copy(w_in.at[at, :], w.at[at, :], more[1].at[k])

    if first:
        for k in range(vocab_rows // block):
            copy(k).start()
    start = 0
    for part in parts:
        at = pl.ds(start, part.shape[0])
        states[at, :] = part[:, :width]
        codes = part[:, width:].astype(F32).astype(jnp.int32)
        ids[at, :] = codes[:, :1] * 256 + codes[:, 1:2]
        start += part.shape[0]
    rows = states.shape[0]
    lane = lax.broadcasted_iota(jnp.int32, (1, 128), 1)

    def step(j, carry):
        top, total, target = carry
        column = pl.multiple_of(j * block, block)
        if first:
            rows_at = pl.ds(column, block)
            pltpu.make_async_copy(w_in.at[rows_at, :], w.at[rows_at, :], more[1].at[j]).wait()
        out = lax.dot_general(
            states[...], w[pl.ds(column, block), :], (((1,), (1,)), ((), ())),
            preferred_element_type=F32,
        ) * (width ** (-0.5))
        logits[:, pl.ds(column, block)] = out
        hits = ids[...] - (here[4] + column)
        lanes = [out[:, k : k + 128] for k in range(0, block, 128)]
        peak = top
        for one in lanes:
            peak = jnp.maximum(peak, one)
        total = total * jnp.exp(top - peak)
        for k, one in enumerate(lanes):
            total = total + jnp.exp(one - peak)
            target = target + jnp.where(hits - k * 128 == lane, one, 0.0)
        return peak, total, target

    zero = jnp.zeros((rows, 128), F32)
    peak, total, target = lax.fori_loop(
        0, vocab_rows // block, step, (jnp.full((rows, 128), -jnp.inf, F32), zero, zero)
    )
    best = jnp.max(peak, axis=1, keepdims=True)
    mass = jnp.sum(total * jnp.exp(peak - best), axis=1, keepdims=True)
    hit = jnp.sum(target, axis=1, keepdims=True)
    mine = jnp.where(lane == 0, best, jnp.where(lane == 1, mass, jnp.where(lane == 2, hit, 0.0)))
    if before < 3:
        table[...] = mine
    else:
        every = jnp.concatenate([one[...] for one in tables[:2]] + [mine])
        table[...] = reordered(every, tables[2][...], ((0,), (0,)))[:8]


def merged(parts):
    top = parts[0][0:1]
    for one in parts[1:]:
        top = jnp.maximum(top, one[0:1])
    total = sum(one[1:2] * jnp.exp(one[0:1] - top) for one in parts)
    return top, total, sum(one[2:3] for one in parts)


def merge_kernel(here, got, out):
    top, total, target = merged([got[k] for k in range(got.shape[0])])
    row = lax.broadcasted_iota(jnp.int32, out.shape[1:], 0)
    stats = jnp.where(row == 0, top, jnp.where(row == 1, total, jnp.where(row == 2, target, 0.0)))
    for k in range(out.shape[0]):
        out[k] = stats


def slab_kernel(own, part, here, *refs):
    got, logits, ids, states, table, outs = refs[0], refs[1:4], refs[4:7], refs[7:10], refs[10], refs[11:]
    loss, log_total, mine, *sent, errors = outs
    width = 4 * part
    top, total, target = merged([got[k] for k in range(got.shape[0])])
    every = top + jnp.log(total)
    row = lax.broadcasted_iota(jnp.int32, got.shape[1:], 0)
    both = jnp.where(row == 0, every, jnp.where(row == 1, every - target, 0.0))
    columns = sum(
        lax.dot_general(table[...], one, (((1,), (1,)), ((), ())), preferred_element_type=F32)
        for one in in_three(both)
    )
    log_total[...] = columns[:, 0:1]
    loss[...] = columns[:own, 1:2]
    strip = mine.shape[0]
    lane = lax.broadcasted_iota(jnp.int32, (1, strip), 1)
    start = 0
    for values, id_part in zip(logits, ids):
        end = start + values.shape[0]
        onehot = (id_part[...] - here[4] == lane).astype(F32)
        part_errors = jnp.exp(values[:, :strip] - columns[start:end, 0:1]) - onehot
        errors[:, start:end] = part_errors.T.astype(BF16)
        start = end

    def grad(k):
        at = pl.multiple_of(lax.rem(here[5] + k, 4) * part, part)
        total, start = 0.0, 0
        for state in states:
            end = start + state.shape[0]
            total += jnp.dot(
                errors[:, start:end], state[:, pl.ds(at, part)], preferred_element_type=F32
            )
            start = end
        return total * (width ** (-0.5))

    for k in (2, 1, 3):
        sent[k - 1][...] = grad(k).astype(BF16)
    mine[...] = grad(0)


def hidden_kernel(other, here, *refs):
    logits, ids, (log_total, w, out, errors) = refs[:3], refs[3:6], refs[6:]
    vocab_rows, width = w.shape
    block, strip = 512, 128
    lane = lax.broadcasted_iota(jnp.int32, (1, strip), 1)
    unit = out.shape[0] // 4
    start = 0
    for values, id_part, parts in zip(logits, ids, GROUPS):
        first = 0
        for whose, line, cell, count in parts:
            last = first + unit * count // 4
            to = line * unit + unit * cell // 4
            if whose == other:
                hits = id_part[first:last, :] - here[4]
                total = log_total[start + first : start + last, :]
                for k in range(0, vocab_rows, strip):
                    onehot = (hits - k == lane).astype(F32)
                    errors[to : to + last - first, k : k + strip] = (
                        jnp.exp(values[first:last, k : k + strip] - total) - onehot
                    ).astype(BF16)
            first = last
        start += first

    def step(j, _):
        cols = pl.ds(pl.multiple_of(j * block, block), block)
        grad = jnp.dot(errors[...], w[:, cols], preferred_element_type=F32) * (width ** (-0.5))
        out[:, cols] = grad.astype(BF16)
        return 0

    lax.fori_loop(0, width // block, step, 0)


def outer_kernel(here, outer, momentum, w0, w1, w2, w3, g0, g1, g2, g3, *outs):
    mean_weight = (to_f32(w0[...]) + to_f32(w1[...]) + to_f32(w2[...]) + to_f32(w3[...])) / 4
    slab_grad = g0[...] + to_f32(g1[...]) + to_f32(g2[...]) + to_f32(g3[...])
    pseudo_grad = outer[...] - (mean_weight - (inner_rate / 4) * slab_grad)
    moved = momentum_coef * momentum[...] + pseudo_grad
    new_outer = outer[...] - outer_rate * (pseudo_grad + momentum_coef * moved)
    if outs[0].dtype == F32:
        outs[0][...], outs[1][...] = new_outer, moved
    else:
        half = outs[0].shape[0]
        outs[0][...], outs[1][...] = new_outer[:half].astype(BF16), new_outer[half:].astype(BF16)


def grad_kernel(here, first, second, third, fourth, *outs):
    rows = outs[0].shape[0]
    for k, out in enumerate(outs):
        at = pl.ds(k * rows, rows)
        value = first[at, :] + to_f32(second[at, :]) + to_f32(third[at, :]) + to_f32(fourth[at, :])
        out[...] = value.astype(out.dtype)


def join_kernel(here, *refs):
    pieces, out = refs[:-1], refs[-1]
    rows = pieces[0].shape[0]
    for k, piece in enumerate(pieces):
        out[k * rows : (k + 1) * rows, :] = piece[...]


def table_kernel(own, here, out):
    out[...] = token_table(here, out.shape[0], own)


def loss_kernel(here, column, row):
    size = column.shape[0]
    at = [lax.broadcasted_iota(jnp.int32, (size, size), dim) for dim in (0, 1)]
    row[...] = jnp.sum(jnp.where(at[0] == at[1], column[...], 0.0), axis=0, keepdims=True)


def place_kernel(part, here, *refs):
    pieces, (pair, sent, out, token_grad, sems) = refs[:8], refs[8:]
    half = pieces[0].shape[0]
    copies = []
    for k, piece in enumerate(pieces):
        at = pl.multiple_of(lax.rem(here[5] + k // 2, 4) * part, part)
        to = out.at[pl.ds(k % 2 * half, half), pl.ds(at, part)]
        copies.append(pltpu.make_async_copy(piece, to, sems.at[k]))
    for one in copies:
        one.start()
    token_grad[...] = pair[: sent.shape[0], :] + to_f32(sent[...])
    for one in copies:
        one.wait()


def per_device(hidden, targets, unembed, outer_weight, momentum):
    weights = unembed[0]
    vocab_rows, width = weights.shape
    own = hidden.shape[1]
    slab_rows, part = outer_weight.shape
    reps = lax.axis_size("rep")
    rep = lax.axis_index("rep")
    tokens = own * lax.axis_size(TOK_VOC)
    group_index = lax.axis_index(TOK) * lax.axis_size(VOC) + lax.axis_index(VOC)
    here = jnp.stack(
        [lax.axis_index(a) for a in TOK_VOC] + [group_index * vocab_rows, rep]
    ).astype(jnp.int32)

    ids = targets[0]
    codes = jnp.stack((ids >> 8, ids & 255), 1).astype(BF16)
    piece = jnp.concatenate((hidden[0], jnp.pad(codes, ((0, 0), (0, 126)))), 1)
    across = take(piece, Z, 1)
    piece = call(join_kernel, shaped(BF16, 2 * own, piece.shape[1]), here, piece, across)
    order = call(functools.partial(table_kernel, own), shaped(BF16, tokens, tokens), here)
    inner = {}
    for k in (2, 1, 3):
        inner[k] = take_inner(piece, k)
    line = call(
        join_kernel, shaped(BF16, 8 * own, piece.shape[1]), here, piece, inner[1], inner[2], inner[3]
    )
    up = take_outer(line, 1)
    down = take_outer(line, -1)
    cut = line.shape[0] // 2
    far_up = take_outer(up[:cut], 1)
    far_down = take_outer(down[cut:], -1)

    def swapped(*parts):
        return [take(one, CORE, 1) for one in parts]

    parts_0 = line, *swapped(line)
    up_swapped, down_swapped = swapped(up, down)
    parts_1 = up, down, up_swapped
    parts_2 = down_swapped, far_up, far_down, *swapped(far_up, far_down)

    def features(value, k):
        return lax.dynamic_slice_in_dim(value, ((rep + k) % reps) * part, part, 1)

    slab = weights[:slab_rows]
    slab_weights = [features(slab, 0)]
    for k in (1, 2, 3):
        slab_weights.append(take(features(slab, -k), "rep", k))

    def logits_of(parts, w, tables):
        rows = sum(one.shape[0] for one in parts)
        out = [
            shaped(F32, rows, vocab_rows),
            shaped(jnp.int32, rows, 1),
            shaped(BF16, rows, width),
            shaped(F32, *((8, tokens) if len(tables) == 3 else (rows, 128))),
        ]
        kind = {}
        if not tables:
            out.append(shaped(BF16, vocab_rows, width))
            kind = dict(
                scratch=[pltpu.SemaphoreType.DMA((4,))],
                specs={len(parts) + 1: pl.BlockSpec(memory_space=pltpu.HBM)},
                limit=40,
            )
        return call(
            functools.partial(logits_kernel, len(parts), len(tables)),
            out, here, *parts, w, *tables,
            flops=2 * max(rows, 256) * vocab_rows * width, **kind,
        )

    logits_0, ids_0, states_0, table_0, w = logits_of(parts_0, weights, ())
    logits_1, ids_1, states_1, table_1 = logits_of(parts_1, w, (table_0,))
    logits_2, ids_2, states_2, stats = logits_of(parts_2, w, (table_0, table_1, order))
    logits, every_id = (logits_0, logits_1, logits_2), (ids_0, ids_1, ids_2)
    states = (states_0, states_1, states_2)

    stats = lax.all_gather(stats, TOK)
    stats = call(merge_kernel, shaped(F32, lax.axis_size(VOC), 4, tokens), here, stats)
    stats = lax.all_to_all(stats, VOC, 0, 0, tiled=True)

    loss, log_total, mine, *grads = call(
        functools.partial(slab_kernel, own, part),
        (
            shaped(F32, own, 1),
            shaped(F32, tokens, 1),
            shaped(F32, slab_rows, part),
            *[shaped(BF16, slab_rows, part)] * 3,
        ),
        here, stats, *logits, *every_id, *states, order,
        flops=2 * tokens * slab_rows * width,
        scratch=[pltpu.VMEM((slab_rows, tokens), BF16)],
    )
    token_loss = call(loss_kernel, shaped(F32, 1, own), here, loss)

    def hidden_terms(other):
        return call(
            functools.partial(hidden_kernel, other), shaped(BF16, tokens // 2, width),
            here, *logits, *every_id, log_total, w,
            flops=tokens * vocab_rows * width,
            scratch=[pltpu.VMEM((tokens // 2, vocab_rows), BF16)],
        )

    send = hidden_terms(1)
    keep = hidden_terms(0)

    slab_grads = [mine, *arrivals(grads, along("rep"))]
    operands = (here, outer_weight, momentum, *slab_weights, *slab_grads)
    rounded = call(outer_kernel, [shaped(BF16, slab_rows // 2, part)] * 2, *operands)
    new_outer, new_momentum = call(outer_kernel, [shaped(F32, slab_rows, part)] * 2, *operands)
    pieces = ring_gather(*rounded, along("rep"))
    got = take(send, CORE, 1)
    total = (to_f32(keep) + to_f32(got)).reshape(4, 8 * own, width)
    rounded = total.astype(BF16)
    got = arrivals(rounded[1:], take_outer)
    pair, *others = call(
        grad_kernel,
        [shaped(F32, 2 * own, width)] + [shaped(BF16, 2 * own, width)] * 3,
        here, total[0], *got,
    )
    for k in (2, 1, 3):
        got = take_inner(others[k - 1], -k)
        pair = pair + to_f32(got)
    pair_sent = take(pair[own:].astype(BF16), Z, 1)
    next_inner, token_grad = call(
        functools.partial(place_kernel, part),
        [shaped(BF16, slab_rows, width), shaped(F32, own, width)],
        here, *pieces, pair, pair_sent,
        scratch=[pltpu.SemaphoreType.DMA((8,))],
        out_spec=[pl.BlockSpec(memory_space=pltpu.HBM), VMEM],
    )
    token_grad = token_grad[None]
    return (token_loss, token_grad, new_outer, new_momentum, next_inner)


def solution(mesh):
    finer = Mesh(
        mesh.devices.reshape(mesh.shape["rep"], 2, 2, 4, 4),
        ("rep", "tok_0", "tok_1", "voc_0", "voc_1"),
    )
    in_specs = (
        P("rep", TOK_VOC, None),
        P("rep", TOK_VOC),
        P("rep", TOK_VOC, None),
        P(TOK_VOC, "rep"),
        P(TOK_VOC, "rep"),
    )
    out_specs = (
        P("rep", TOK_VOC),
        P("rep", TOK_VOC, None),
        P(TOK_VOC, "rep"),
        P(TOK_VOC, "rep"),
        P(TOK_VOC, None),
    )

    return jax.shard_map(per_device, mesh=finer, in_specs=in_specs, out_specs=out_specs, check_vma=False)
```
